256 devices in a mesh: dp: 8 (over z), section: 2 (over core), space: 16 (over y, x).
Axes of the slice: x: 4, y: 4, z: 8, core: 2. Of those that a mesh axis runs over, the one named last changes fastest.
Arguments:
- latents: bfloat16 [32, 96, 192, 320], P('dp', 'space'), parts along dimension 0, may hold values from -16 to 16
- kernels: bfloat16 [2, 3, 3, 320, 320], P('section'), may hold values from -0.109375 to 0.109375
- norm_gain: float32 [2, 320], P('section'), may hold values from 0.25 to 1.75
- norm_bias: float32 [2, 320], P('section'), may hold values from -3 to 3
- conv_bias: float32 [2, 320], P('section'), may hold values from -3 to 3
Outputs:
- skips: bfloat16 [2, 32, 96, 192, 320], P('section', 'dp', 'space'), parts along dimension 1
The draws below stay inside these ranges and needn't reach their ends.
There are 8 independent parts, one for each index of `dp`. The reference program is written for one: setup_inputs(seed, part) draws one part's arguments, and reference() takes and returns one part's arrays. A program takes and returns all parts, laid end to end along the dimension named above; an argument that names none is the same for every part. Nothing has to cross between parts.
All inputs are finite; a program needn't handle non-finite values.
Results may differ from the reference program's by a relative error of at most 0.01.
Values may be sent and summed in bfloat16 or wider, within the bound.
A program may use at most 128 MiB of HBM per device.

```python
import jax
import jax.numpy as jnp
from jax import lax

C = 320
GROUPS = 32
H = 96
W = 192
MICRO = 4
SECTIONS = 2


def draw_latents(key, part):
    noise_key = jax.random.fold_in(key, 101)
    offset_key = jax.random.fold_in(key, 202)
    positions = jnp.arange(H, dtype=jnp.float32) / (H - 1)
    base = jax.random.normal(noise_key, (MICRO, H, W, C), jnp.float32)
    scales = 0.4 * jnp.exp(jnp.log(3.0) * positions)
    ramp = 0.3 * jnp.exp(jnp.log(10.0) * positions)
    offsets = 0.6 * jax.random.normal(offset_key, (MICRO, 1, 1, C), jnp.float32) + 1.0
    values = base * scales[None, :, None, None] + offsets * ramp[None, :, None, None]
    return jnp.clip(values, -16.0, 16.0).astype(jnp.bfloat16)


def block_levels(stream_key, dims, shards, least, largest):
    level, own = 1.0, jax.random.fold_in(stream_key, 6)
    for axis_at, shards_of in shards:
        heights = jnp.exp(jax.random.uniform(jax.random.fold_in(own, axis_at), (shards_of,), jnp.float32, least / len(shards), largest / len(shards)))
        level = level * jnp.repeat(heights, dims[axis_at] // shards_of).reshape([-1 if axis == axis_at else 1 for axis in range(len(dims))])
    return level


def gaussian(key, dims, scale, reach, cuts=(), held_as=jnp.bfloat16):
    level = block_levels(key, dims, cuts, -0.22, 0.18) if cuts else 1.0
    result = jax.random.normal(key, dims, jnp.float32) * scale * level
    return jnp.minimum(jnp.maximum(result, -reach), reach).astype(held_as)


def setup_inputs(seed: int = 0, part: int = 0) -> dict:
    splits = jax.random.split(jax.random.key(seed), 6)
    own_keys = jax.random.split(jax.random.fold_in(splits[5], part), 6)
    return {
        "latents": draw_latents(jax.random.fold_in(jax.random.fold_in(splits[5], part), 71), part),
        "kernels": gaussian(splits[1], (SECTIONS, 3, 3, C, C), (9 * C) ** -0.5, 0.109375, ((0, 2),)),
        "norm_gain": jnp.clip(1.0 + 0.15 * jax.random.normal(splits[2], (SECTIONS, C), jnp.float32), 0.25, 1.75),
        "norm_bias": gaussian(splits[3], (SECTIONS, C), 0.5, 3.0, ((0, 2),), jnp.float32),
        "conv_bias": gaussian(splits[4], (SECTIONS, C), 0.5, 3.0, ((0, 2),), jnp.float32),
    }


def group_norm_silu(inputs, norm_gain, norm_shift):
    batch_count = inputs.shape[0]
    values = inputs.astype(jnp.float32).reshape(batch_count, H * W, GROUPS, C // GROUPS)
    group_mean = lax.optimization_barrier(jnp.mean(values, axis=(1, 3), keepdims=True))
    deviation = values - group_mean
    group_var = lax.optimization_barrier(jnp.mean(deviation * deviation, axis=(1, 3), keepdims=True))
    scaled = (deviation * lax.rsqrt(group_var + 1e-05)).reshape(batch_count, H, W, C)
    scaled = scaled * norm_gain + norm_shift
    return jax.nn.silu(scaled).astype(jnp.bfloat16)

def convolve(normed, kernel):
    return lax.conv_general_dilated(normed, kernel, (1, 1), ((1, 1), (1, 1)), dimension_numbers=('NHWC', 'HWIO', 'NHWC'), preferred_element_type=jnp.float32)

def reference(latents, kernels, norm_gain, norm_bias, conv_bias):
    normed_first = group_norm_silu(latents, norm_gain[0], norm_bias[0])
    first = (convolve(normed_first, kernels[0]) + conv_bias[0]).astype(jnp.bfloat16)
    normed_second = group_norm_silu(first, norm_gain[1], norm_bias[1])
    second = (latents.astype(jnp.float32) + convolve(normed_second, kernels[1]) + conv_bias[1]).astype(jnp.bfloat16)
    return jnp.stack([first, second])
```

```python
import jax
import jax.numpy as jnp
from jax import lax
from jax.experimental import pallas as pl
from jax.experimental.pallas import tpu as pltpu
from jax.sharding import PartitionSpec as P

GROUPS = 32
EPS = 1e-5
F32 = jnp.float32
BF16 = jnp.bfloat16
MESH = pl.DeviceIdType.MESH
MAIN = 256
STEP = 16


def three_parts(row):
    high = row.astype(BF16)
    rest = row - high.astype(F32)
    middle = rest.astype(BF16)
    low = (rest - middle.astype(F32)).astype(BF16)
    return [high.astype(F32), middle.astype(F32), low.astype(F32)]


def stacked_parts(first, second):
    rows = three_parts(first) + three_parts(second)
    rows.append(jnp.zeros((10, first.shape[1]), F32))
    return jnp.concatenate(rows, axis=0).astype(BF16)


def make_kernel(n_space, samples, rows, columns, channels):
    half = rows // 2
    tail = channels - MAIN
    per_group = channels // GROUPS
    chunks = columns // STEP
    members = rows * n_space * columns * per_group
    peers = 2 * n_space

    def kernel(
        lat, ker, gain, bias, cbias, out,
        x_ref, w_ref, wt_ref, par_ref, f_ref, s_ref, y_ref, am_ref, pt_ref,
        g_ref, gt_ref, st0, st1, ab_ref,
        sem_x, sem_w, sem_p, sem_ws, sem_wr, sem_ps, sem_pr,
        sem_h0s, sem_h0r, sem_t0s, sem_t0r, sem_t1s, sem_t1r,
        sem_ds, sem_dr, sem_h1s, sem_h1r, sem_ol, sem_os, sem_or,
    ):
        space = lax.axis_index("space")
        sec = lax.axis_index("section")
        other = 1 - sec
        me = space * 2 + sec
        has_edge = jnp.logical_or(
            jnp.logical_and(sec == 0, space > 0),
            jnp.logical_and(sec == 1, space < n_space - 1),
        )
        beside = jnp.clip(space + 2 * sec - 1, 0, n_space - 1)
        partner = {"section": other}

        barrier = pltpu.get_barrier_semaphore()

        def greet(j, c):
            p = lax.rem(me + j, peers)
            pl.semaphore_signal(
                barrier, inc=1,
                device_id={"space": p // 2, "section": lax.rem(p, 2)},
                device_id_type=MESH,
            )
            return c

        lax.fori_loop(1, peers, greet, 0)

        def x_copy(b):
            return pltpu.make_async_copy(lat.at[b], x_ref.at[b, pl.ds(1, rows)], sem_x.at[b])

        small = (gain, bias, cbias)

        def p_copy(i):
            return pltpu.make_async_copy(small[i], par_ref.at[sec, i], sem_p.at[i])

        w_copy = pltpu.make_async_copy(ker.at[0], w_ref.at[sec], sem_w)
        for b in range(samples):
            x_copy(b).start()
        w_copy.start()
        for i in range(3):
            p_copy(i).start()

        shape = (channels, 128)
        low = lax.broadcasted_iota(jnp.int32, shape, 1) * per_group
        at = lax.broadcasted_iota(jnp.int32, shape, 0)
        g_ref[...] = jnp.where(jnp.logical_and(at >= low, at < low + per_group), 1.0, 0.0).astype(BF16)
        shape = (128, channels)
        low = lax.broadcasted_iota(jnp.int32, shape, 0) * per_group
        at = lax.broadcasted_iota(jnp.int32, shape, 1)
        gt_ref[...] = jnp.where(jnp.logical_and(at >= low, at < low + per_group), 1.0, 0.0).astype(BF16)

        pl.semaphore_wait(barrier, peers - 1)

        def h0_copy(b):
            return pltpu.make_async_remote_copy(
                lat.at[b, (rows - 1) * sec], x_ref.at[b, (rows + 1) * other],
                sem_h0s.at[b], sem_h0r.at[b],
                device_id={"space": beside, "section": other}, device_id_type=MESH,
            )

        w_send = pltpu.make_async_remote_copy(
            ker.at[0], w_ref.at[sec], sem_ws, sem_wr, device_id=partner, device_id_type=MESH
        )

        def p_send(i):
            return pltpu.make_async_remote_copy(
                small[i], par_ref.at[sec, i], sem_ps.at[i], sem_pr.at[i],
                device_id=partner, device_id_type=MESH,
            )

        @pl.when(has_edge)
        def _():
            for b in range(samples):
                h0_copy(b).start()

        for i in range(3):
            p_send(i).start()
        w_send.start()

        def group_sums(sums):
            s_m, s_t, q_m, q_t = [jnp.sum(v, axis=0, keepdims=True) for v in sums]
            total = jnp.zeros((16, 128), F32)
            for s, q, start, size in ((s_m, q_m, 0, MAIN), (s_t, q_t, MAIN, tail)):
                total += jnp.dot(
                    stacked_parts(s, q), g_ref[pl.ds(start, size), :], preferred_element_type=F32
                )
            return jnp.concatenate(
                [total[0:1] + total[1:2] + total[2:3], total[3:4] + total[4:5] + total[5:6]], axis=0
            )

        def folded(v):
            return v[0:8] + v[8:16]

        def zero_sums():
            return (
                jnp.zeros((8, MAIN), F32), jnp.zeros((8, tail), F32),
                jnp.zeros((8, MAIN), F32), jnp.zeros((8, tail), F32),
            )

        def added(sums, m, t):
            return (
                sums[0] + folded(m), sums[1] + folded(t),
                sums[2] + folded(m * m), sums[3] + folded(t * t),
            )

        def t0_send(b, j):
            return pltpu.make_async_remote_copy(
                st0.at[b, space], st0.at[b, space], sem_t0s.at[b], sem_t0r.at[b],
                device_id={"space": lax.rem(space + j, n_space)}, device_id_type=MESH,
            )

        def input_stats(b, c):
            x_copy(b).wait()

            def row(r, sums):
                for k in range(chunks):
                    at = pl.ds(k * STEP, STEP)
                    m = x_ref[b, r, at, 0:MAIN].astype(F32)
                    t = x_ref[b, r, at, MAIN:channels].astype(F32)
                    sums = added(sums, m, t)
                return sums

            st0[b, space] = group_sums(lax.fori_loop(1, rows + 1, row, zero_sums()))

            def send(j, c):
                t0_send(b, j).start()
                return c

            lax.fori_loop(1, n_space, send, 0)
            return c

        lax.fori_loop(0, samples, input_stats, 0)

        def affine(layer, totals):
            mean = totals[0:1] * (1.0 / members)
            var = jnp.maximum(totals[1:2] * (1.0 / members) - mean * mean, 0.0)
            inv = lax.rsqrt(var + EPS)
            parts = stacked_parts(inv, mean * inv)
            spread = jnp.dot(parts, gt_ref[...], preferred_element_type=F32)
            inv_c = spread[0:1] + spread[1:2] + spread[2:3]
            shift_c = spread[3:4] + spread[4:5] + spread[5:6]
            g = par_ref[layer, 0]
            ab_ref[0:1, :] = inv_c * g * 0.5
            ab_ref[1:2, :] = (par_ref[layer, 1] - shift_c * g) * 0.5

        def norm_row(src, dst):
            a_m, a_t = ab_ref[0:1, 0:MAIN], ab_ref[0:1, MAIN:channels]
            b_m, b_t = ab_ref[1:2, 0:MAIN], ab_ref[1:2, MAIN:channels]

            def act(k):
                at = pl.ds(k * STEP, STEP)
                h = src[at, 0:MAIN].astype(F32) * a_m + b_m
                m = h + h * jnp.tanh(h)
                h = src[at, MAIN:channels].astype(F32) * a_t + b_t
                return m, h + h * jnp.tanh(h)

            none = (jnp.zeros((8, MAIN), F32), jnp.zeros((8, tail), F32))
            before, now = none, act(0)
            zeros = jnp.zeros((STEP, 256 - 3 * tail), F32)
            for k in range(chunks):
                later = act(k + 1) if k < chunks - 1 else None
                head = none if later is None else (later[0][0:8], later[1][0:8])
                wide = [jnp.concatenate([p, n, h], axis=0) for p, n, h in zip(before, now, head)]
                at = pl.ds(k * STEP, STEP)
                dst[at, 0:256] = wide[0][7:23].astype(BF16)
                dst[at, 256:512] = now[0].astype(BF16)
                dst[at, 512:768] = wide[0][9:25].astype(BF16)
                dst[at, 768:1024] = jnp.concatenate(
                    [wide[1][7:23], now[1], wide[1][9:25], zeros], axis=1
                ).astype(BF16)
                before, now = (now[0][8:16], now[1][8:16]), later

        def norm_all(src_of):
            def row(j, c):
                i = j + 1 - sec
                norm_row(src_of(i), y_ref.at[i])
                return c

            lax.fori_loop(0, half + 1, row, 0)
            edge = (half + 1) * sec

            @pl.when(has_edge)
            def _():
                norm_row(src_of(edge), y_ref.at[edge])

            @pl.when(jnp.logical_not(has_edge))
            def _():
                y_ref[edge] = jnp.zeros((columns, 1024), BF16)

        def pack_tail(layer):
            for dc in range(3):
                taps = [w_ref[layer, dr, dc, :, MAIN:channels].astype(F32) for dr in range(3)]
                taps.append(jnp.zeros((channels, 256 - 3 * tail), F32))
                packed = jnp.concatenate(taps, axis=1).astype(BF16)
                wt_ref[pl.ds(dc * MAIN, MAIN), :] = packed[0:MAIN]
                wt_ref[pl.ds(3 * MAIN + dc * tail, tail), :] = packed[MAIN:channels]
            wt_ref[pl.ds(3 * MAIN + 3 * tail, 256 - 3 * tail), :] = jnp.zeros((256 - 3 * tail, 256), BF16)

        def convolve(layer):
            pieces = []
            for dr in range(3):
                tiles = [w_ref[layer, dr, dc, 0:MAIN, 0:MAIN] for dc in range(3)]
                tiles += [w_ref[layer, dr, dc, MAIN:channels, 0:MAIN] for dc in range(3)]
                tiles.append(jnp.zeros((256 - 3 * tail, MAIN), BF16))
                pieces.append(jnp.concatenate(tiles, axis=0))
            for r in range(half):
                acc = None
                for dr in range(3):
                    part = jnp.dot(y_ref[r + dr], pieces[dr], preferred_element_type=F32)
                    acc = part if acc is None else acc + part
                am_ref[r] = acc
            for i in range(half + 2):
                pt_ref[i] = jnp.dot(y_ref[i], wt_ref[...], preferred_element_type=F32)

        def conv_out(r, at):
            m = am_ref[r, at, :]
            t = (
                pt_ref[r, at, 0:tail]
                + pltpu.roll(pt_ref[r + 1, at, 0:128], 64, 1)[:, 0:tail]
                + pt_ref[r + 2, at, 128 : 128 + tail]
            )
            return m, t

        def out_move(layer, b, ref):
            span = pl.ds(half * sec, half)
            local = pltpu.make_async_copy(ref, out.at[0, b, span], sem_ol.at[b])
            remote = pltpu.make_async_remote_copy(
                ref, out.at[0, b, span], sem_os.at[b], sem_or.at[b],
                device_id=partner, device_id_type=MESH,
            )
            return local, remote

        def first_view(b):
            return f_ref.at[b, pl.ds(1, half)]

        def out_start(layer, b, ref):
            local, remote = out_move(layer, b, ref)

            @pl.when(sec == layer)
            def _():
                local.start()

            @pl.when(sec != layer)
            def _():
                remote.start()

        def t1_send(b, j):
            p = lax.rem(me + j, peers)
            return pltpu.make_async_remote_copy(
                st1.at[b, me], st1.at[b, me], sem_t1s.at[b], sem_t1r.at[b],
                device_id={"space": p // 2, "section": lax.rem(p, 2)}, device_id_type=MESH,
            )

        def d_send(b):
            return pltpu.make_async_remote_copy(
                f_ref.at[b, half - (half - 1) * sec], f_ref.at[b, (half + 1) * sec],
                sem_ds.at[b], sem_dr.at[b], device_id=partner, device_id_type=MESH,
            )

        def h1_send(b):
            return pltpu.make_async_remote_copy(
                f_ref.at[b, 1 + (half - 1) * sec], f_ref.at[b, (half + 1) * other],
                sem_h1s.at[b], sem_h1r.at[b],
                device_id={"space": beside, "section": other}, device_id_type=MESH,
            )

        def all_bytes(ref, b, count, sem):
            view = ref.at[b, pl.ds(0, count)]
            return pltpu.make_async_copy(view, view, sem.at[b])

        w_copy.wait()
        for i in range(3):
            p_copy(i).wait()
        for i in range(3):
            p_send(i).wait()
        w_send.wait()

        pack_tail(0)

        def first_stage(b, c):
            @pl.when(has_edge)
            def _():
                h0_copy(b).wait_recv()

            all_bytes(st0, b, n_space - 1, sem_t0r).wait()
            affine(0, jnp.sum(st0[b], axis=0))
            base = half * sec
            norm_all(lambda i: x_ref.at[b, base + i])
            convolve(0)
            cb = par_ref[0, 2]

            def row(r, sums):
                for k in range(chunks):
                    at = pl.ds(k * STEP, STEP)
                    m, t = conv_out(r, at)
                    m = (m + cb[:, 0:MAIN]).astype(BF16)
                    t = (t + cb[:, MAIN:channels]).astype(BF16)
                    f_ref[b, 1 + r, at, 0:MAIN] = m
                    f_ref[b, 1 + r, at, MAIN:channels] = t
                    sums = added(sums, m.astype(F32), t.astype(F32))
                return sums

            sums = lax.fori_loop(0, half, row, zero_sums())
            st1[b, me] = group_sums(sums)

            def send(j, c):
                t1_send(b, j).start()
                return c

            lax.fori_loop(1, peers, send, 0)
            d_send(b).start()

            @pl.when(has_edge)
            def _():
                h1_send(b).start()

            out_start(0, b, first_view(b))
            return c

        lax.fori_loop(0, samples, first_stage, 0)

        pack_tail(1)

        def second_stage(b, c):
            d_send(b).wait_recv()

            @pl.when(has_edge)
            def _():
                h1_send(b).wait_recv()

            all_bytes(st1, b, peers - 1, sem_t1r).wait()
            affine(1, jnp.sum(st1[b], axis=0))
            norm_all(lambda i: f_ref.at[b, i])
            convolve(1)
            cb = par_ref[1, 2]

            def row(r, c):
                for k in range(chunks):
                    at = pl.ds(k * STEP, STEP)
                    m, t = conv_out(r, at)
                    xr = x_ref.at[b, 1 + half * sec + r]
                    m = m + xr[at, 0:MAIN].astype(F32) + cb[:, 0:MAIN]
                    t = t + xr[at, MAIN:channels].astype(F32) + cb[:, MAIN:channels]
                    s_ref[b, r, at, 0:MAIN] = m.astype(BF16)
                    s_ref[b, r, at, MAIN:channels] = t.astype(BF16)
                return c

            lax.fori_loop(0, half, row, 0)

            out_start(1, b, s_ref.at[b])
            return c

        lax.fori_loop(0, samples, second_stage, 0)

        def finish(b, c):
            @pl.when(has_edge)
            def _():
                h0_copy(b).wait_send()
                h1_send(b).wait_send()

            all_bytes(st0, b, n_space - 1, sem_t0s).wait()
            all_bytes(st1, b, peers - 1, sem_t1s).wait()
            d_send(b).wait_send()
            local, remote = out_move(0, b, first_view(b))
            local.wait()
            remote.wait_send()
            remote.wait_recv()
            return c

        lax.fori_loop(0, samples, finish, 0)

    dma = pltpu.SemaphoreType.DMA
    per_sample = dma((samples,))
    scratch = [
        pltpu.VMEM((samples, rows + 2, columns, channels), BF16),
        pltpu.VMEM((2, 3, 3, channels, channels), BF16),
        pltpu.VMEM((1024, 256), BF16),
        pltpu.VMEM((2, 3, 1, channels), F32),
        pltpu.VMEM((samples, half + 2, columns, channels), BF16),
        pltpu.VMEM((samples, half, columns, channels), BF16),
        pltpu.VMEM((half + 2, columns, 1024), BF16),
        pltpu.VMEM((half, columns, MAIN), F32),
        pltpu.VMEM((half + 2, columns, 256), F32),
        pltpu.VMEM((channels, 128), BF16),
        pltpu.VMEM((128, channels), BF16),
        pltpu.VMEM((samples, n_space, 2, 128), F32),
        pltpu.VMEM((samples, peers, 2, 128), F32),
        pltpu.VMEM((8, channels), F32),
        per_sample, dma, dma((3,)), dma, dma, dma((3,)), dma((3,)),
        per_sample, per_sample, per_sample, per_sample, per_sample, per_sample,
        per_sample, per_sample, per_sample, per_sample, per_sample, per_sample, per_sample,
    ]
    return kernel, scratch


def solution(mesh):
    n_space = mesh.shape["space"]

    def on_device(latents, kernels, norm_gain, norm_bias, conv_bias):
        samples, rows, columns, channels = latents.shape
        kernel, scratch = make_kernel(n_space, samples, rows, columns, channels)
        return pl.pallas_call(
            kernel,
            out_shape=jax.ShapeDtypeStruct((1, samples, rows, columns, channels), BF16),
            in_specs=[pl.BlockSpec(memory_space=pl.ANY)] * 5,
            out_specs=pl.BlockSpec(memory_space=pl.ANY),
            scratch_shapes=scratch,
            compiler_params=pltpu.CompilerParams(
                collective_id=0, has_side_effects=True, vmem_limit_bytes=56 * 1024 * 1024
            ),
            name="resblock",
        )(latents, kernels, norm_gain, norm_bias, conv_bias)

    return jax.shard_map(
        on_device,
        mesh=mesh,
        in_specs=(
            P("dp", "space", None, None),
            P("section", None, None, None, None),
            P("section", None),
            P("section", None),
            P("section", None),
        ),
        out_specs=P("section", "dp", "space", None, None),
        check_vma=False,
    )
```

```python
import jax
import jax.numpy as jnp
from jax import lax
from jax.experimental import pallas as pl
from jax.experimental.pallas import tpu as pltpu
from jax.sharding import PartitionSpec as P

GROUPS = 32
EPS = 1e-5
F32 = jnp.float32
BF16 = jnp.bfloat16
MESH = pl.DeviceIdType.MESH
MAIN = 256
STEP = 16


def three_parts(row):
    high = row.astype(BF16)
    rest = row - high.astype(F32)
    middle = rest.astype(BF16)
    low = (rest - middle.astype(F32)).astype(BF16)
    return [high.astype(F32), middle.astype(F32), low.astype(F32)]


def stacked_parts(first, second):
    rows = three_parts(first) + three_parts(second)
    rows.append(jnp.zeros((10, first.shape[1]), F32))
    return jnp.concatenate(rows, axis=0).astype(BF16)


def make_kernel(n_space, samples, rows, columns, channels):
    half = rows // 2
    tail = channels - MAIN
    per_group = channels // GROUPS
    chunks = columns // STEP
    members = rows * n_space * columns * per_group
    peers = 2 * n_space
    stages = 2 * samples

    def kernel(
        lat, ker, gain, bias, cbias, out,
        x_ref, w_ref, wt_ref, par_ref, f_ref, s_ref, ya_ref, yb_ref, ta_ref, tb_ref, am_ref, pt_ref,
        g_ref, gt_ref, st_ref,
        sem_x, sem_w, sem_p, sem_ws, sem_wr, sem_ps, sem_pr,
        sem_hs, sem_hr, sem_ts, sem_tr, sem_ds, sem_dr, sem_ol, sem_os, sem_or,
    ):
        space = lax.axis_index("space")
        sec = lax.axis_index("section")
        other = 1 - sec
        me = space * 2 + sec
        at_top = jnp.logical_and(sec == 0, space == 0)
        at_bottom = jnp.logical_and(sec == 1, space == n_space - 1)
        has_edge = jnp.logical_not(jnp.logical_or(at_top, at_bottom))
        beside = jnp.clip(space + 2 * sec - 1, 0, n_space - 1)
        partner = {"section": other}

        barrier = pltpu.get_barrier_semaphore()

        def everyone():
            for j in range(n_space):
                there = lax.rem(space + j, n_space) if j else space
                for t in (0, 1):
                    if j or t:
                        yield {"space": there, "section": other if t else sec}

        for peer in everyone():
            pl.semaphore_signal(barrier, inc=1, device_id=peer, device_id_type=MESH)

        def x_copy(b):
            return pltpu.make_async_copy(
                lat.at[b, pl.ds((half - 1) * sec, half + 1)],
                x_ref.at[b, pl.ds(other, half + 1)], sem_x.at[b],
            )

        small = (gain, bias, cbias)

        def p_copy(i):
            return pltpu.make_async_copy(small[i], par_ref.at[sec, i], sem_p.at[i])

        w_copy = pltpu.make_async_copy(ker.at[0], w_ref.at[sec], sem_w)
        for b in range(samples):
            x_copy(b).start()
        w_copy.start()
        for i in range(3):
            p_copy(i).start()

        shape = (channels, 128)
        low = lax.broadcasted_iota(jnp.int32, shape, 1) * per_group
        at = lax.broadcasted_iota(jnp.int32, shape, 0)
        g_ref[...] = jnp.where(jnp.logical_and(at >= low, at < low + per_group), 1.0, 0.0).astype(BF16)
        shape = (128, channels)
        low = lax.broadcasted_iota(jnp.int32, shape, 0) * per_group
        at = lax.broadcasted_iota(jnp.int32, shape, 1)
        gt_ref[...] = jnp.where(jnp.logical_and(at >= low, at < low + per_group), 1.0, 0.0).astype(BF16)
        pt_ref[...] = jnp.zeros_like(pt_ref)
        ta_ref[...] = jnp.zeros_like(ta_ref)
        tb_ref[...] = jnp.zeros_like(tb_ref)

        @pl.when(jnp.logical_not(has_edge))
        def _():
            def clear(b, c):
                x_ref[b, (half + 1) * sec] = jnp.zeros((columns, channels), BF16)
                f_ref[b, (half + 1) * sec] = jnp.zeros((columns, channels), BF16)
                return c

            lax.fori_loop(0, samples, clear, 0)

        def group_sums(sums):
            s_m, s_t, q_m, q_t = [jnp.sum(v, axis=0, keepdims=True) for v in sums]
            total = jnp.zeros((16, 128), F32)
            for s, q, start, size in ((s_m, q_m, 0, MAIN), (s_t, q_t, MAIN, tail)):
                total += jnp.dot(
                    stacked_parts(s, q), g_ref[pl.ds(start, size), :], preferred_element_type=F32
                )
            return jnp.concatenate(
                [total[0:1] + total[1:2] + total[2:3], total[3:4] + total[4:5] + total[5:6]], axis=0
            )

        def folded(v):
            return v[0:8] + v[8:16]

        def zero_sums():
            return (
                jnp.zeros((8, MAIN), F32), jnp.zeros((8, tail), F32),
                jnp.zeros((8, MAIN), F32), jnp.zeros((8, tail), F32),
            )

        def added(sums, m, t):
            return (
                sums[0] + folded(m), sums[1] + folded(t),
                sums[2] + folded(m * m), sums[3] + folded(t * t),
            )

        def input_stats(b, c):
            x_copy(b).wait()

            def row(r, sums):
                for k in range(chunks):
                    at = pl.ds(k * STEP, STEP)
                    m = x_ref[b, r, at, 0:MAIN].astype(F32)
                    t = x_ref[b, r, at, MAIN:channels].astype(F32)
                    sums = added(sums, m, t)
                return sums

            st_ref[b, me] = group_sums(lax.fori_loop(1, half + 1, row, zero_sums()))
            return c

        lax.fori_loop(0, samples, input_stats, 0)

        def pack_tail(layer):
            for dr in range(3):
                taps = [w_ref[layer, dr, dc, :, MAIN:channels].astype(F32) for dc in range(3)]
                taps.append(jnp.zeros((channels, 256 - 3 * tail), F32))
                packed = jnp.concatenate(taps, axis=1).astype(BF16)
                wt_ref[layer, pl.ds(dr * MAIN, MAIN), :] = packed[0:MAIN]
                wt_ref[layer, pl.ds(3 * MAIN + dr * tail, tail), :] = packed[MAIN:channels]
            wt_ref[layer, pl.ds(3 * MAIN + 3 * tail, 256 - 3 * tail), :] = jnp.zeros(
                (256 - 3 * tail, 256), BF16
            )

        w_copy.wait()
        for i in range(3):
            p_copy(i).wait()
        pack_tail(sec)

        pl.semaphore_wait(barrier, peers - 1)

        def t_sends(k):
            return [
                pltpu.make_async_remote_copy(
                    st_ref.at[k, me], st_ref.at[k, me], sem_ts.at[k], sem_tr.at[k],
                    device_id=peer, device_id_type=MESH,
                )
                for peer in everyone()
            ]

        def halo(k):
            ref = x_ref if k < samples else f_ref
            b = k % samples
            return pltpu.make_async_remote_copy(
                ref.at[b, 1 + (half - 1) * sec], ref.at[b, (half + 1) * other],
                sem_hs.at[k], sem_hr.at[k],
                device_id={"space": beside, "section": other}, device_id_type=MESH,
            )

        w_send = pltpu.make_async_remote_copy(
            w_ref.at[sec], w_ref.at[sec], sem_ws, sem_wr, device_id=partner, device_id_type=MESH
        )

        def p_send(i):
            return pltpu.make_async_remote_copy(
                par_ref.at[sec, i], par_ref.at[sec, i], sem_ps.at[i], sem_pr.at[i],
                device_id=partner, device_id_type=MESH,
            )

        for i in range(3):
            p_send(i).start()
        w_send.start()
        for k in range(samples):
            for copy in t_sends(k):
                copy.start()

            @pl.when(has_edge)
            def _(k=k):
                halo(k).start()

        def affine(k):
            layer = k // samples
            totals = jnp.sum(st_ref[k], axis=0)
            mean = totals[0:1] * (1.0 / members)
            var = jnp.maximum(totals[1:2] * (1.0 / members) - mean * mean, 0.0)
            inv = lax.rsqrt(var + EPS)
            spread = jnp.dot(
                stacked_parts(inv, mean * inv), gt_ref[...], preferred_element_type=F32
            )
            inv_c = spread[0:1] + spread[1:2] + spread[2:3]
            shift_c = spread[3:4] + spread[4:5] + spread[5:6]
            g = par_ref[layer, 0]
            a = inv_c * g * 0.5
            return a, (par_ref[layer, 1] - shift_c * g) * 0.5

        top_keep = jnp.where(at_top, 0.0, 1.0)
        bottom_keep = jnp.where(at_bottom, 0.0, 1.0)

        def norm_row(k, i, ab, y, t):
            ref = x_ref if k < samples else f_ref
            b = k % samples
            a, s = ab
            if i == 0:
                a, s = a * top_keep, s * top_keep
            if i == half + 1:
                a, s = a * bottom_keep, s * bottom_keep
            a_m, a_t, b_m, b_t = a[:, 0:MAIN], a[:, MAIN:], s[:, 0:MAIN], s[:, MAIN:]

            def act(c):
                at = pl.ds(c * STEP, STEP)
                h = ref[b, i, at, 0:MAIN].astype(F32) * a_m + b_m
                m = h + h * jnp.tanh(h)
                h = ref[b, i, at, MAIN:channels].astype(F32) * a_t + b_t
                return m, h + h * jnp.tanh(h)

            none = (jnp.zeros((8, MAIN), F32), jnp.zeros((8, tail), F32))
            before, now = none, act(0)
            zeros = jnp.zeros((STEP, 256 - 3 * tail), F32)
            for c in range(chunks):
                later = act(c + 1) if c < chunks - 1 else None
                after = none if later is None else (later[0][0:8], later[1][0:8])
                wide = [jnp.concatenate([p, n, h], axis=0) for p, n, h in zip(before, now, after)]
                at = pl.ds(c * STEP, STEP)
                y[i, at, 0:256] = wide[0][7:23].astype(BF16)
                y[i, at, 256:512] = now[0].astype(BF16)
                y[i, at, 512:768] = wide[0][9:25].astype(BF16)
                packed = jnp.concatenate(
                    [wide[1][7:23], now[1], wide[1][9:25], zeros], axis=1
                ).astype(BF16)
                y[i, at, 768:1024] = packed
                own = now[1].astype(BF16)
                if i < half:
                    t[i, at, 0:tail] = own
                if 1 <= i <= half:
                    t[i - 1, at, tail : 2 * tail] = packed[:, tail : 2 * tail]
                if i >= 2:
                    t[i - 2, at, 2 * tail : 3 * tail] = own
                before, now = (now[0][8:16], now[1][8:16]), later

        def stage(k):
            layer, b = k // samples, k % samples
            y, t = ((ya_ref, ta_ref), (yb_ref, tb_ref))[k % 2]
            y_next, t_next = ((yb_ref, tb_ref), (ya_ref, ta_ref))[k % 2]
            more = k + 1 < stages
            if more:
                ab = affine(k + 1)
            for r in range(half):
                lhs = jnp.concatenate([y[r + dr, :, 256:512] for dr in range(3)] + [t[r]], axis=1)
                pt_ref[r, pl.ds(8, columns), :] = jnp.dot(
                    lhs, wt_ref[layer], preferred_element_type=F32
                )
            tiles = []
            for dr in range(3):
                tiles += [w_ref[layer, dr, dc, 0:MAIN, 0:MAIN] for dc in range(3)]
                tiles += [w_ref[layer, dr, dc, MAIN:channels, 0:MAIN] for dc in range(3)]
                tiles.append(jnp.zeros((256 - 3 * tail, MAIN), BF16))
            weights = jnp.concatenate(tiles, axis=0)
            cb = par_ref[layer, 2]
            sums = zero_sums()
            norms = list(range(half + 2))
            for r in range(half):
                lhs = jnp.concatenate([y[r + dr] for dr in range(3)], axis=1)
                am_ref[r] = jnp.dot(lhs, weights, preferred_element_type=F32)
                if more:
                    for i in norms[2 * r : 2 * r + 2]:
                        norm_row(k + 1, i, ab, y_next, t_next)
            for r in range(half):
                for c in range(chunks):
                    at = pl.ds(c * STEP, STEP)
                    m = am_ref[r, at, :] + cb[:, 0:MAIN]
                    wide = pt_ref[r, pl.ds(c * STEP, STEP + 16), :]
                    u = (
                        wide[7:23, 0:tail]
                        + pltpu.roll(wide[8:24, 0:128], 64, 1)[:, 0:tail]
                        + wide[9:25, 128 : 128 + tail]
                        + cb[:, MAIN:channels]
                    )
                    if layer == 0:
                        m, u = m.astype(BF16), u.astype(BF16)
                        f_ref[b, 1 + r, at, 0:MAIN] = m
                        f_ref[b, 1 + r, at, MAIN:channels] = u
                        sums = added(sums, m.astype(F32), u.astype(F32))
                    else:
                        m = m + x_ref[b, 1 + r, at, 0:MAIN].astype(F32)
                        u = u + x_ref[b, 1 + r, at, MAIN:channels].astype(F32)
                        s_ref[b, r, at, 0:MAIN] = m.astype(BF16)
                        s_ref[b, r, at, MAIN:channels] = u.astype(BF16)
            if layer == 0:
                st_ref[k + samples, me] = group_sums(sums)

        def out_move(layer, b):
            ref = f_ref.at[b, pl.ds(1, half)] if layer == 0 else s_ref.at[b]
            span = pl.ds(half * sec, half)
            local = pltpu.make_async_copy(ref, out.at[0, b, span], sem_ol.at[b])
            remote = pltpu.make_async_remote_copy(
                ref, out.at[0, b, span], sem_os.at[b], sem_or.at[b],
                device_id=partner, device_id_type=MESH,
            )
            return local, remote

        def out_start(layer, b):
            local, remote = out_move(layer, b)

            @pl.when(sec == layer)
            def _():
                local.start()

            @pl.when(sec != layer)
            def _():
                remote.start()

        def d_send(b):
            return pltpu.make_async_remote_copy(
                f_ref.at[b, half - (half - 1) * sec], f_ref.at[b, (half + 1) * sec],
                sem_ds.at[b], sem_dr.at[b], device_id=partner, device_id_type=MESH,
            )

        def all_bytes(k, sem):
            view = st_ref.at[k, pl.ds(0, peers - 1)]
            return pltpu.make_async_copy(view, view, sem.at[k])

        def arrived(k):
            if k >= samples:
                d_send(k - samples).wait_recv()

            @pl.when(has_edge)
            def _():
                halo(k).wait_recv()

            all_bytes(k, sem_tr).wait()

        for i in range(3):
            p_send(i).wait()
        arrived(0)
        ab = affine(0)
        for i in range(half + 2):
            norm_row(0, i, ab, ya_ref, ta_ref)
        w_send.wait()
        pack_tail(other)

        for k in range(stages):
            if k + 1 < stages:
                arrived(k + 1)
            stage(k)
            layer, b = k // samples, k % samples
            if layer == 0:
                for copy in t_sends(k + samples):
                    copy.start()
                d_send(b).start()

                @pl.when(has_edge)
                def _(k=k):
                    halo(k + samples).start()

            out_start(layer, b)

        for k in range(stages):
            @pl.when(has_edge)
            def _(k=k):
                halo(k).wait_send()

            all_bytes(k, sem_ts).wait()
        for b in range(samples):
            d_send(b).wait_send()
            local, remote = out_move(0, b)
            local.wait()
            remote.wait_send()
            remote.wait_recv()

    dma = pltpu.SemaphoreType.DMA
    each, both = dma((samples,)), dma((2 * samples,))
    scratch = [
        pltpu.VMEM((samples, half + 2, columns, channels), BF16),
        pltpu.VMEM((2, 3, 3, channels, channels), BF16),
        pltpu.VMEM((2, 1024, 256), BF16),
        pltpu.VMEM((2, 3, 1, channels), F32),
        pltpu.VMEM((samples, half + 2, columns, channels), BF16),
        pltpu.VMEM((samples, half, columns, channels), BF16),
        pltpu.VMEM((half + 2, columns, 1024), BF16),
        pltpu.VMEM((half + 2, columns, 1024), BF16),
        pltpu.VMEM((half, columns, 256), BF16),
        pltpu.VMEM((half, columns, 256), BF16),
        pltpu.VMEM((half, columns, MAIN), F32),
        pltpu.VMEM((half, columns + 16, 256), F32),
        pltpu.VMEM((channels, 128), BF16),
        pltpu.VMEM((128, channels), BF16),
        pltpu.VMEM((2 * samples, peers, 2, 128), F32),
        each, dma, dma((3,)), dma, dma, dma((3,)), dma((3,)),
        both, both, both, both, each, each, each, each, each,
    ]
    return kernel, scratch


def solution(mesh):
    n_space = mesh.shape["space"]

    def on_device(latents, kernels, norm_gain, norm_bias, conv_bias):
        samples, rows, columns, channels = latents.shape
        kernel, scratch = make_kernel(n_space, samples, rows, columns, channels)
        return pl.pallas_call(
            kernel,
            out_shape=pltpu.VMEM((1, samples, rows, columns, channels), BF16),
            in_specs=[pl.BlockSpec(memory_space=pl.ANY)] * 5,
            out_specs=pl.BlockSpec(memory_space=pltpu.VMEM),
            scratch_shapes=scratch,
            compiler_params=pltpu.CompilerParams(
                collective_id=0, has_side_effects=True, vmem_limit_bytes=56 * 1024 * 1024
            ),
            name="resblock",
        )(latents, kernels, norm_gain, norm_bias, conv_bias)

    return jax.shard_map(
        on_device,
        mesh=mesh,
        in_specs=(
            P("dp", "space", None, None),
            P("section", None, None, None, None),
            P("section", None),
            P("section", None),
            P("section", None),
        ),
        out_specs=P("section", "dp", "space", None, None),
        check_vma=False,
    )
```

```python
import jax
import jax.numpy as jnp
from jax import lax
from jax.experimental import pallas as pl
from jax.experimental.pallas import tpu as pltpu
from jax.sharding import PartitionSpec as P

GROUPS = 32
EPS = 1e-5
F32 = jnp.float32
BF16 = jnp.bfloat16
MESH = pl.DeviceIdType.MESH
MAIN = 256
ORDER = (0, 3, 2, 1)
SPLIT = (1, 9)
STEP = 16


def three_parts(row):
    high = row.astype(BF16)
    rest = row - high.astype(F32)
    middle = rest.astype(BF16)
    low = (rest - middle.astype(F32)).astype(BF16)
    return [high.astype(F32), middle.astype(F32), low.astype(F32)]


def stacked_parts(first, second):
    rows = three_parts(first) + three_parts(second)
    rows.append(jnp.zeros((10, first.shape[1]), F32))
    return jnp.concatenate(rows, axis=0).astype(BF16)


def make_kernel(n_space, samples, rows, columns, channels):
    half = rows // 2
    tail = channels - MAIN
    per_group = channels // GROUPS
    chunks = columns // STEP
    members = rows * n_space * columns * per_group
    peers = 2 * n_space
    stages = 2 * samples

    def kernel(
        lat, ker, gain, bias, cbias, out,
        x_ref, w_ref, wt_ref, par_ref, f_ref, ya_ref, yb_ref, yc_ref, t_ref, am_ref, pt_ref,
        e_ref, g_ref, gt_ref, st_ref,
        sem_x, sem_w, sem_p, sem_ws, sem_wr, sem_ps, sem_pr,
        sem_hs, sem_hr, sem_ts, sem_tr, sem_ds, sem_dr, sem_os, sem_or,
    ):
        space = lax.axis_index("space")
        sec = lax.axis_index("section")
        other = 1 - sec
        me = space * 2 + sec
        at_top = jnp.logical_and(sec == 0, space == 0)
        at_bottom = jnp.logical_and(sec == 1, space == n_space - 1)
        has_edge = jnp.logical_not(jnp.logical_or(at_top, at_bottom))
        beside = jnp.clip(space + 2 * sec - 1, 0, n_space - 1)
        partner = {"section": other}

        load_base = space // n_space
        store_base = me // peers

        barrier = pltpu.get_barrier_semaphore()

        def everyone():
            for j in range(n_space):
                there = lax.rem(space + j, n_space) if j else space
                for t in (0, 1):
                    if j or t:
                        yield {"space": there, "section": other if t else sec}

        for peer in everyone():
            pl.semaphore_signal(barrier, inc=1, device_id=peer, device_id_type=MESH)

        def x_copy(b):
            return pltpu.make_async_copy(
                lat.at[b, pl.ds((half - 1) * sec, half + 1)],
                x_ref.at[b, pl.ds(other, half + 1)], sem_x.at[b],
            )

        small = (gain, bias, cbias)

        def p_copy(i):
            return pltpu.make_async_copy(small[i], par_ref.at[sec, i], sem_p.at[i])

        w_copy = pltpu.make_async_copy(ker.at[0], w_ref.at[sec], sem_w)
        for b in range(samples):
            x_copy(b).start()
        w_copy.start()
        for i in range(3):
            p_copy(i).start()

        shape = (channels, 128)
        low = lax.broadcasted_iota(jnp.int32, shape, 1) * per_group
        at = lax.broadcasted_iota(jnp.int32, shape, 0)
        g_ref[...] = jnp.where(jnp.logical_and(at >= low, at < low + per_group), 1.0, 0.0).astype(BF16)
        shape = (128, channels)
        low = lax.broadcasted_iota(jnp.int32, shape, 0) * per_group
        at = lax.broadcasted_iota(jnp.int32, shape, 1)
        gt_ref[...] = jnp.where(jnp.logical_and(at >= low, at < low + per_group), 1.0, 0.0).astype(BF16)
        edge = jnp.zeros((8, 128), F32)
        for ref, count in ((e_ref, 3 * (half + 2)), (pt_ref, 2 * half)):
            for i in range(count):
                ref[i, 0:8, :] = edge
                ref[i, pl.ds(columns + 8, 8), :] = edge

        @pl.when(jnp.logical_not(has_edge))
        def _():
            def clear(b, c):
                x_ref[b, (half + 1) * sec] = jnp.zeros((columns, channels), BF16)
                f_ref[b, (half + 1) * sec] = jnp.zeros((columns, channels), BF16)
                return c

            lax.fori_loop(0, samples, clear, 0)

        def group_sums(sums):
            s_m, s_t, q_m, q_t = [jnp.sum(v, axis=0, keepdims=True) for v in sums]
            total = jnp.zeros((16, 128), F32)
            for s, q, start, size in ((s_m, q_m, 0, MAIN), (s_t, q_t, MAIN, tail)):
                total += jnp.dot(
                    stacked_parts(s, q), g_ref[pl.ds(start, size), :], preferred_element_type=F32
                )
            return jnp.concatenate(
                [total[0:1] + total[1:2] + total[2:3], total[3:4] + total[4:5] + total[5:6]], axis=0
            )

        def folded(v):
            return v[0:8] + v[8:16]

        def zero_sums():
            return (
                jnp.zeros((8, MAIN), F32), jnp.zeros((8, tail), F32),
                jnp.zeros((8, MAIN), F32), jnp.zeros((8, tail), F32),
            )

        def added(sums, m, t):
            return (
                sums[0] + folded(m), sums[1] + folded(t),
                sums[2] + folded(m * m), sums[3] + folded(t * t),
            )

        def input_stats(b, c):
            x_copy(b).wait()

            def row(r, sums):
                for k in range(chunks):
                    at = pl.ds(k * STEP, STEP)
                    m = x_ref[b, r, at, 0:MAIN].astype(F32)
                    t = x_ref[b, r, at, MAIN:channels].astype(F32)
                    sums = added(sums, m, t)
                return sums

            st_ref[b, me] = group_sums(lax.fori_loop(1, half + 1, row, zero_sums()))
            return c

        lax.fori_loop(0, samples, input_stats, 0)

        def pack_tail(layer):
            for dr in range(3):
                taps = [w_ref[layer, dr, dc, :, MAIN:channels].astype(F32) for dc in range(3)]
                taps.append(jnp.zeros((channels, 256 - 3 * tail), F32))
                packed = jnp.concatenate(taps, axis=1).astype(BF16)
                wt_ref[layer, pl.ds(dr * MAIN, MAIN), :] = packed[0:MAIN]
                wt_ref[layer, pl.ds(3 * MAIN + dr * tail, tail), :] = packed[MAIN:channels]
            wt_ref[layer, pl.ds(3 * MAIN + 3 * tail, 256 - 3 * tail), :] = jnp.zeros(
                (256 - 3 * tail, 256), BF16
            )

        w_copy.wait()
        for i in range(3):
            p_copy(i).wait()
        pack_tail(sec)

        pl.semaphore_wait(barrier, peers - 1)

        def t_sends(k):
            return [
                pltpu.make_async_remote_copy(
                    st_ref.at[k, me], st_ref.at[k, me], sem_ts.at[k], sem_tr.at[k],
                    device_id=peer, device_id_type=MESH,
                )
                for peer in everyone()
            ]

        def halo(k):
            ref = x_ref if k < samples else f_ref
            b = k % samples
            return pltpu.make_async_remote_copy(
                ref.at[b, 1 + (half - 1) * sec], ref.at[b, (half + 1) * other],
                sem_hs.at[k], sem_hr.at[k],
                device_id={"space": beside, "section": other}, device_id_type=MESH,
            )

        w_send = pltpu.make_async_remote_copy(
            w_ref.at[sec], w_ref.at[sec], sem_ws, sem_wr, device_id=partner, device_id_type=MESH
        )

        def p_send(i):
            return pltpu.make_async_remote_copy(
                par_ref.at[sec, i], par_ref.at[sec, i], sem_ps.at[i], sem_pr.at[i],
                device_id=partner, device_id_type=MESH,
            )

        for i in range(3):
            p_send(i).start()
        w_send.start()
        for k in range(samples):
            for copy in t_sends(k):
                copy.start()

            @pl.when(has_edge)
            def _(k=k):
                halo(k).start()

        def affine(k):
            layer = k // samples
            totals = jnp.sum(st_ref[k], axis=0)
            mean = totals[0:1] * (1.0 / members)
            var = jnp.maximum(totals[1:2] * (1.0 / members) - mean * mean, 0.0)
            inv = lax.rsqrt(var + EPS)
            spread = jnp.dot(
                stacked_parts(inv, mean * inv), gt_ref[...], preferred_element_type=F32
            )
            inv_c = spread[0:1] + spread[1:2] + spread[2:3]
            shift_c = spread[3:4] + spread[4:5] + spread[5:6]
            g = par_ref[layer, 0]
            a = inv_c * g * 0.5
            return a, (par_ref[layer, 1] - shift_c * g) * 0.5

        top_keep = jnp.where(at_top, 0.0, 1.0)
        bottom_keep = jnp.where(at_bottom, 0.0, 1.0)

        def norm_row(k, i, ab):
            ref = x_ref if k < samples else f_ref
            b = k % samples
            y = (ya_ref, yb_ref)[k % 2]
            slot = store_base + k % 2
            a, s = ab
            if i == 0:
                a, s = a * top_keep, s * top_keep
            if i == half + 1:
                a, s = a * bottom_keep, s * bottom_keep
            a_m, a_t, b_m, b_t = a[:, 0:MAIN], a[:, MAIN:], s[:, 0:MAIN], s[:, MAIN:]

            low_lanes = lax.broadcasted_iota(jnp.int32, (STEP, 128), 1) < tail

            for c in range(chunks):
                at = pl.ds(c * STEP, STEP)
                inside = pl.ds(8 + c * STEP, STEP)
                out_at = pl.ds(i * columns + c * STEP, STEP)
                h = ref[b, i, at, 0:MAIN].astype(F32) * a_m + b_m
                m = h + h * jnp.tanh(h)
                h = ref[b, i, at, MAIN:channels].astype(F32) * a_t + b_t
                u = h + h * jnp.tanh(h)
                u = jnp.concatenate([u, u], axis=1)
                yc_ref[slot, out_at, :] = m.astype(BF16)
                e_ref[3 * i, inside, :] = m[:, 0:128]
                e_ref[3 * i + 1, inside, :] = m[:, 128:256]
                e_ref[3 * i + 2, inside, :] = u
                own = u.astype(BF16)
                if i < half:
                    t_ref[slot, pl.ds(i * columns + c * STEP, STEP), 0:tail] = own[:, 0:tail]
                if 1 <= i <= half:
                    t_ref[slot, pl.ds((i - 1) * columns + c * STEP, STEP), tail : 2 * tail] = own[:, tail : 2 * tail]
                if i >= 2:
                    t_ref[slot, pl.ds((i - 2) * columns + c * STEP, STEP), 128:256] = own
            for c in range(chunks):
                out_at = pl.ds(i * columns + c * STEP, STEP)
                for p in range(2):
                    lanes = pl.ds(128 * p, 128)
                    y[0, out_at, lanes] = e_ref[3 * i + p, pl.ds(7 + c * STEP, STEP), :].astype(BF16)
                    y[2, out_at, lanes] = e_ref[3 * i + p, pl.ds(9 + c * STEP, STEP), :].astype(BF16)
                before = e_ref[3 * i + 2, pl.ds(7 + c * STEP, STEP), :]
                now = e_ref[3 * i + 2, pl.ds(8 + c * STEP, STEP), :]
                after = e_ref[3 * i + 2, pl.ds(9 + c * STEP, STEP), :]
                y[1, out_at, 0:128] = jnp.where(low_lanes, before, now).astype(BF16)
                y[1, out_at, 128:256] = after.astype(BF16)

        def stage(k):
            layer, b = k // samples, k % samples
            y = (ya_ref, yb_ref)[k % 2]
            slot = load_base + k % 2
            more = k + 1 < stages
            block = half * columns // 2

            def rows_of(q, dr, d):
                at = pl.ds(dr * columns + d * block, block)
                if q == 1:
                    return yc_ref[slot, at, :]
                return y[(0, None, 2, 1)[q], at, :]

            order = [(q, dr) for q in ORDER for dr in range(3)]
            tiles = []
            for q, dr in order:
                if q < 3:
                    tiles.append(w_ref[layer, dr, q, 0:MAIN, 0:MAIN])
                else:
                    tiles += [w_ref[layer, dr, dc, MAIN:channels, 0:MAIN] for dc in range(3)]
                    tiles.append(jnp.zeros((256 - 3 * tail, MAIN), BF16))
            weights = jnp.concatenate(tiles, axis=0)
            cb = par_ref[layer, 2]
            def main_dots(first, last):
                for d in range(2):
                    lhs = jnp.concatenate([rows_of(q, dr, d) for q, dr in order[first:last]], axis=1)
                    part = jnp.dot(
                        lhs, weights[MAIN * first : MAIN * last], preferred_element_type=F32
                    )
                    at = pl.ds(d * block, block)
                    am_ref[at, :] = part if first == 0 else am_ref[at, :] + part

            main_dots(0, SPLIT[0])
            if more:
                ab = affine(k + 1)
                for i in range(half + 2):
                    norm_row(k + 1, i, ab)
            main_dots(SPLIT[0], SPLIT[1])
            main_dots(SPLIT[1], 12)
            mine = sec if layer == 0 else other
            s_m, s_t, q_m, q_t = zero_sums()
            for r in range(half):
                for c in range(chunks):
                    at = pl.ds(c * STEP, STEP)
                    m = am_ref[pl.ds(r * columns + c * STEP, STEP), :] + cb[:, 0:MAIN]
                    if layer == 0:
                        m = m.astype(BF16)
                        f_ref[b, 1 + r, at, 0:MAIN] = m
                        v = m.astype(F32)
                        s_m, q_m = s_m + folded(v), q_m + folded(v * v)
                    else:
                        m = (m + x_ref[b, 1 + r, at, 0:MAIN].astype(F32)).astype(BF16)
                    out[mine, b, half * sec + r, at, 0:MAIN] = m
            for d in range(2):
                lhs = jnp.concatenate(
                    [rows_of(1, dr, d) for dr in range(3)] + [t_ref[slot, pl.ds(d * block, block), :]], axis=1
                )
                part = jnp.dot(lhs, wt_ref[layer], preferred_element_type=F32)
                for h in range(3):
                    r, start = divmod((3 * d + h) * (columns // 2), columns)
                    piece = part[h * (columns // 2) : (h + 1) * (columns // 2)]
                    pt_ref[2 * r, pl.ds(8 + start, columns // 2), :] = piece[:, 0:128]
                    pt_ref[2 * r + 1, pl.ds(8 + start, columns // 2), :] = piece[:, 128:256]
            for r in range(half):
                for c in range(chunks):
                    at = pl.ds(c * STEP, STEP)
                    u = (
                        pt_ref[2 * r, pl.ds(7 + c * STEP, STEP), :]
                        + pltpu.roll(pt_ref[2 * r, pl.ds(8 + c * STEP, STEP), :], 64, 1)
                        + pt_ref[2 * r + 1, pl.ds(9 + c * STEP, STEP), :]
                    )[:, 0:tail] + cb[:, MAIN:channels]
                    if layer == 0:
                        u = u.astype(BF16)
                        f_ref[b, 1 + r, at, MAIN:channels] = u
                        v = u.astype(F32)
                        s_t, q_t = s_t + folded(v), q_t + folded(v * v)
                    else:
                        u = (u + x_ref[b, 1 + r, at, MAIN:channels].astype(F32)).astype(BF16)
                    out[mine, b, half * sec + r, at, MAIN:channels] = u
            sums = (s_m, s_t, q_m, q_t)
            if layer == 0:
                st_ref[k + samples, me] = group_sums(sums)

        def out_send(b):
            span = pl.ds(half * sec, half)
            return pltpu.make_async_remote_copy(
                out.at[1, b, span], out.at[0, b, span], sem_os.at[b], sem_or.at[b],
                device_id=partner, device_id_type=MESH,
            )

        def d_send(b):
            return pltpu.make_async_remote_copy(
                f_ref.at[b, half - (half - 1) * sec], f_ref.at[b, (half + 1) * sec],
                sem_ds.at[b], sem_dr.at[b], device_id=partner, device_id_type=MESH,
            )

        def all_bytes(k, sem):
            view = st_ref.at[k, pl.ds(0, peers - 1)]
            return pltpu.make_async_copy(view, view, sem.at[k])

        def arrived(k):
            if k >= samples:
                d_send(k - samples).wait_recv()

            @pl.when(has_edge)
            def _():
                halo(k).wait_recv()

            all_bytes(k, sem_tr).wait()

        for i in range(3):
            p_send(i).wait()
        arrived(0)
        ab = affine(0)
        for i in range(half + 2):
            norm_row(0, i, ab)
        w_send.wait()
        pack_tail(other)

        for k in range(stages):
            if k + 1 < stages:
                arrived(k + 1)
            stage(k)
            layer, b = k // samples, k % samples
            if layer == 0:
                for copy in t_sends(k + samples):
                    copy.start()
                d_send(b).start()

                @pl.when(has_edge)
                def _(k=k):
                    halo(k + samples).start()

            @pl.when(sec != layer)
            def _(b=b):
                out_send(b).start()

        for k in range(stages):
            @pl.when(has_edge)
            def _(k=k):
                halo(k).wait_send()

            all_bytes(k, sem_ts).wait()
        for b in range(samples):
            d_send(b).wait_send()
            out_send(b).wait()

    dma = pltpu.SemaphoreType.DMA
    each, both = dma((samples,)), dma((2 * samples,))
    scratch = [
        pltpu.VMEM((samples, half + 2, columns, channels), BF16),
        pltpu.VMEM((2, 3, 3, channels, channels), BF16),
        pltpu.VMEM((2, 1024, 256), BF16),
        pltpu.VMEM((2, 3, 1, channels), F32),
        pltpu.VMEM((samples, half + 2, columns, channels), BF16),
        pltpu.VMEM((3, (half + 2) * columns, 256), BF16),
        pltpu.VMEM((3, (half + 2) * columns, 256), BF16),
        pltpu.VMEM((2, (half + 2) * columns, 256), BF16),
        pltpu.VMEM((2, half * columns, 256), BF16),
        pltpu.VMEM((half * columns, MAIN), F32),
        pltpu.VMEM((2 * half, columns + 16, 128), F32),
        pltpu.VMEM((3 * (half + 2), columns + 16, 128), F32),
        pltpu.VMEM((channels, 128), BF16),
        pltpu.VMEM((128, channels), BF16),
        pltpu.VMEM((2 * samples, peers, 2, 128), F32),
        each, dma, dma((3,)), dma, dma, dma((3,)), dma((3,)),
        both, both, both, both, each, each, each, each,
    ]
    return kernel, scratch


def solution(mesh):
    n_space = mesh.shape["space"]

    def on_device(latents, kernels, norm_gain, norm_bias, conv_bias):
        samples, rows, columns, channels = latents.shape
        kernel, scratch = make_kernel(n_space, samples, rows, columns, channels)
        both = pl.pallas_call(
            kernel,
            out_shape=pltpu.VMEM((2, samples, rows, columns, channels), BF16),
            in_specs=[pl.BlockSpec(memory_space=pl.ANY)] * 5,
            out_specs=pl.BlockSpec(memory_space=pltpu.VMEM),
            scratch_shapes=scratch,
            compiler_params=pltpu.CompilerParams(
                collective_id=0,
                has_side_effects=True, vmem_limit_bytes=56 * 1024 * 1024
            ),
            name="resblock",
        )(latents, kernels, norm_gain, norm_bias, conv_bias)
        return both[0:1]

    return jax.shard_map(
        on_device,
        mesh=mesh,
        in_specs=(
            P("dp", "space", None, None),
            P("section", None, None, None, None),
            P("section", None),
            P("section", None),
            P("section", None),
        ),
        out_specs=P("section", "dp", "space", None, None),
        check_vma=False,
    )
```
